512 devices in a mesh: param: 64 (over x_hi, z, core), qoi: 8 (over x_lo, y).
Axes of the slice: x: 4 (x_hi: 2, x_lo: 2; x = x_hi * 2 + x_lo), y: 4, z: 16, core: 2. Of those that a mesh axis runs over, the one named last changes fastest.
Arguments:
- samples: bfloat16 [64, 20480, 420], P('qoi', 'param'), may hold values from -16 to 16
- operator_rows: bfloat16 [8, 20480, 2, 2048], P(None, 'param', None, 'qoi'), may hold values from -0.03125 to 0.03125
- block_start: int32 [1], replicated, may hold values from 0 to 203
- gauge_group: int32 [2048], P('qoi'), may hold values from 0 to 15
Outputs:
- qoi_spectrum: float32 [64, 2, 8, 2048], P('param', None, None, 'qoi')
- segment_response: float32 [64, 2, 8, 16], P('param')
The draws below stay inside these ranges and needn't reach their ends.
Inputs may be any that keep to these rules, and one draw needn't show every extreme that they name: `block_start`: the block's frequencies lie among the 211 frequencies of a real transform.
All inputs are finite; a program needn't handle non-finite values.
Results may differ from the reference program's by a relative error of at most 0.005.
Values may be sent and summed in bfloat16 or wider, within the bound.
A program may use at most 64 MiB of HBM per device.

```python
import math
import jax
import jax.numpy as jnp
from jax import lax

NF = 8
NT = 420
GROUPS = 16
SAMPLES = 64
NP = 20480
GAUGES = 2048


def place_ends(result, rng, least, largest):
    longest = result.shape.index(max(result.shape))
    spots = []
    for shift in (0, 1):
        where = [jax.random.randint(jax.random.fold_in(rng, axis), (), 0, length) for axis, length in enumerate(result.shape)]
        where[longest] = (where[longest] + shift) % result.shape[longest]
        spots.append(tuple(where))
    return result.at[spots[0]].set(least).at[spots[1]].set(largest)


def raised(result, own_key, source, target, shards_of, factor):
    owner, partner = [(jnp.arange(result.shape[dim]) // (result.shape[dim] // shards_of)).reshape([-1 if axis == dim else 1 for axis in range(result.ndim)]) for dim in (source, target)]
    chosen = jax.random.permutation(own_key, shards_of)[partner]
    strong = (owner == chosen) | (owner == (partner + shards_of // 2) % shards_of)
    return jnp.where(strong, factor * result, result)


def block_scale(own_key, extent, split, least, largest):
    def one(dim, shards_of):
        steps = jax.random.uniform(jax.random.fold_in(jax.random.fold_in(own_key, 6), dim), (shards_of,), jnp.float32, least / len(split), largest / len(split))
        return jnp.repeat(jnp.exp(steps), extent[dim] // shards_of).reshape((-1,) + (1,) * (len(extent) - dim - 1))

    loudness = one(*split[0])
    for cut in split[1:]:
        loudness = loudness * one(*cut)
    return loudness


def noise(rng, shape, width, most, shards=(), held_as=jnp.bfloat16):
    loudness = block_scale(rng, shape, shards, -0.22, 0.18) if shards else 1.0
    drawn = jax.random.normal(rng, shape, jnp.float32) * width * loudness
    return jnp.minimum(jnp.maximum(drawn, -most), most).astype(held_as)


def gaussian_with(key, dims, scale, reach, split, heavy, kind=jnp.bfloat16):
    array = scale * jax.random.normal(key, dims, jnp.float32)
    if split:
        array = array * block_scale(key, dims, split, -0.22, 0.18)
    return jnp.clip(raised(array, jax.random.fold_in(key, 3), *heavy), -reach, reach).astype(kind)


def setup_inputs(seed: int = 0) -> dict:
    key_of = jax.random.split(jax.random.key(seed), 5)
    return {
        "samples": gaussian_with(key_of[0], (SAMPLES, NP, NT), 1.0, 16.0, ((0, 8), (1, 64)), (1, 0, 64, 4.0)),
        "operator_rows": noise(key_of[1], (NF, NP, 2, GAUGES), (2 * NP) ** -0.5, 0.03125, ((1, 64), (3, 8))),
        "block_start": jax.random.randint(key_of[2], (1,), 0, NT // 2 + 2 - NF).astype(jnp.int32),
        "gauge_group": place_ends(jax.random.randint(key_of[3], (GAUGES,), 0, GROUPS), jax.random.fold_in(key_of[3], 1), 0, GROUPS - 1).astype(jnp.int32),
    }


def sample_spectrum(series, first):
    spectrum_all = jnp.fft.rfft(series.astype(jnp.float32), axis=-1)
    window = lax.dynamic_slice_in_dim(spectrum_all, first, NF, 1)
    factor = 1.0 / math.sqrt(NT)
    real_part = (jnp.real(window) * factor).astype(jnp.bfloat16)
    imag_part = (jnp.imag(window) * factor).astype(jnp.bfloat16)
    return jnp.stack([real_part, imag_part], axis=0)

def frequency_response(paired):
    spectrum_f, weights_f = paired
    real_w = weights_f[:, 0, :]
    imag_w = weights_f[:, 1, :]
    real_real = jnp.dot(spectrum_f[0], real_w, preferred_element_type=jnp.float32)
    imag_imag = jnp.dot(spectrum_f[1], imag_w, preferred_element_type=jnp.float32)
    real_imag = jnp.dot(spectrum_f[0], imag_w, preferred_element_type=jnp.float32)
    imag_real = jnp.dot(spectrum_f[1], real_w, preferred_element_type=jnp.float32)
    return jnp.stack([real_real - imag_imag, real_imag + imag_real], axis=0)

def reference(samples, operator_rows, block_start, gauge_group):
    first = block_start[0].astype(jnp.int32)
    spectra = lax.map(lambda series: sample_spectrum(series, first), samples)
    spectra = jnp.transpose(spectra, (3, 1, 0, 2))
    responses = lax.map(frequency_response, (spectra, operator_rows))
    qoi_spectrum = jnp.transpose(responses, (2, 1, 0, 3))
    onehot = (gauge_group[:, None] == jnp.arange(GROUPS, dtype=jnp.int32)[None, :]).astype(jnp.float32)
    segment = jnp.dot(qoi_spectrum.reshape(-1, GAUGES), onehot, precision=lax.Precision.HIGHEST, preferred_element_type=jnp.float32)
    segment_response = segment.reshape(SAMPLES, 2, NF, GROUPS) * math.sqrt(GROUPS / GAUGES)
    return (qoi_spectrum, segment_response)
```

```python
import functools
import math

import jax
import jax.numpy as jnp
from jax import lax
from jax.experimental import pallas as pl
from jax.experimental.pallas import tpu as pltpu
from jax.sharding import PartitionSpec as P

GROUPS = 16
MESH = pl.DeviceIdType.MESH
BF = jnp.bfloat16
F32 = jnp.float32

NQ = 8
NX = 2
NZ = 16
NF = 8
NT = 420
NS = 8
NP = 320
NG = 256
LANES = 2 * NP
STEPS = ((0, 100), (100, 128), (228, 96), (324, 96))
NEAR = 4


def owner_offsets():
    pairs = [(dx, dz) for dx in range(NX) for dz in range(-NZ // 2 + 1, NZ // 2 + 1) if (dx, dz) != (0, 0)]
    return sorted(pairs, key=lambda pair: (-(abs(pair[1]) + 2 * pair[0]), -pair[1]))


def phase_rows(first, begin, width):
    lane = lax.broadcasted_iota(jnp.int32, (NF, width), 1) + begin
    freq = lax.broadcasted_iota(jnp.int32, (NF, width), 0) + first
    turns = ((lane >> 3) * freq).astype(F32)
    rest = turns - NT * jnp.floor(turns * (1.0 / NT))
    quarter = jnp.floor(rest * (4.0 / NT) + 0.5)
    angle = (rest - (NT // 4) * quarter) * (2.0 * math.pi / NT)
    sq = angle * angle
    sine = angle * (1.0 + sq * (-1.0 / 6 + sq * (1.0 / 120 + sq * (-1.0 / 5040 + sq * (1.0 / 362880)))))
    cosine = 1.0 + sq * (-0.5 + sq * (1.0 / 24 + sq * (-1.0 / 720 + sq * (1.0 / 40320 + sq * (-1.0 / 3628800)))))
    odd = (quarter == 1.0) | (quarter == 3.0)
    scale = 1.0 / math.sqrt(NT)
    cos_all = jnp.where(odd, sine, cosine) * jnp.where((quarter == 1.0) | (quarter == 2.0), -scale, scale)
    sin_all = jnp.where(odd, cosine, sine) * jnp.where((quarter == 2.0) | (quarter == 3.0), scale, -scale)
    return cos_all, sin_all


def fill_table(first, core, rows_ref, table_ref):
    full = NT * NS
    for begin in range(0, full, 512):
        width = min(512, full - begin)
        rows_ref[0, :, begin : begin + width], rows_ref[1, :, begin : begin + width] = phase_rows(first, begin, width)
    for begin in range(0, full, 512):
        width = min(512, full - begin)
        span = slice(begin, begin + width)
        sample = lax.broadcasted_iota(jnp.int32, (16, width), 1) % NS
        row = lax.broadcasted_iota(jnp.int32, (16, width), 0)
        member = row // 8
        side = jnp.where(member == 0, core, 1 - core)
        hit = sample == (row % 4) * 2 + side
        upper = (row % 8) // 4 == 1
        for part in range(2):
            for pair in range(NF // 2):
                low = jnp.broadcast_to(rows_ref[part, 2 * pair : 2 * pair + 1, span], (16, width))
                high = jnp.broadcast_to(rows_ref[part, 2 * pair + 1 : 2 * pair + 2, span], (16, width))
                value = jnp.where(hit, jnp.where(upper, high, low), 0.0)
                rounded = value.astype(BF)
                at = part * 64 + pair * 16
                table_ref[at : at + 16, span] = rounded
                table_ref[128 + at : 144 + at, span] = (value - rounded.astype(F32)).astype(BF)


def planar(f, w_ref, order_ref, out_ref):
    for begin in range(0, NP, 128):
        count = min(128, NP - begin)
        rows = w_ref[f, begin : begin + count].reshape(2 * count, NG)
        order = order_ref[0] if count == 128 else order_ref[1, : 2 * count, : 2 * count]
        out_ref[f, 2 * begin : 2 * (begin + count)] = jnp.dot(order, rows, preferred_element_type=F32).astype(BF)


def kernel(
    x_hbm, w_hbm, first_hbm, group_hbm, acc_out, seg_out,
    x_v, table, rows, w_v, w_p, order, spectra, give, take, own, spread, send, recv, segs, first_s, group_v,
    x_sem, w_sem, first_sem, group_sem, ag_send, ag_recv, core_send, core_recv, rs_send, rs_recv, seg_send, seg_recv,
    far, line,
):
    pi, qj = lax.axis_index("param"), lax.axis_index("qoi")
    core, chip = pi % 2, pi // 2
    xh, z = chip // NZ, chip % NZ

    def param_at(dx, dz, dc=0):
        return (((xh + dx) % NX) * NZ + (z + dz + NZ) % NZ) * 2 + (core + dc) % 2

    first_copy = pltpu.make_async_copy(first_hbm, first_s, first_sem)
    first_copy.start()
    x_copies = [
        pltpu.make_async_copy(x_hbm.at[pl.ds(t0, n)], x_v.at[pl.ds(t0, n)], x_sem.at[i]) for i, (t0, n) in enumerate(STEPS)
    ]
    for copy in x_copies:
        copy.start()
    w_copy = pltpu.make_async_copy(w_hbm, w_v, w_sem)
    w_copy.start()
    group_copy = pltpu.make_async_copy(group_hbm, group_v, group_sem)
    group_copy.start()

    barrier = pltpu.get_barrier_semaphore()
    near = [(param_at(0, dz), qj) for dz in range(-NEAR, NEAR + 1) if dz]
    near += [(param_at(1, 0), qj), (param_at(0, 0, 1), qj)]
    near += [(pi, (qj + d) % NQ) for d in range(1, NQ)]
    for peer in near:
        pl.semaphore_signal(barrier, inc=1, device_id=peer, device_id_type=MESH)

    big = lax.broadcasted_iota(jnp.int32, (256, 256), 0)
    col = lax.broadcasted_iota(jnp.int32, (256, 256), 1)
    order[0] = jnp.where(col == (big % 128) * 2 + big // 128, 1.0, 0.0).astype(BF)
    order[1] = jnp.where(col == (big % 64) * 2 + (big // 64) % 2, 1.0, 0.0).astype(BF)

    first_copy.wait()
    fill_table(first_s[0], core, rows, table)

    halves = jnp.zeros((256, NP), F32)
    for copy, (t0, n) in zip(x_copies, STEPS):
        copy.wait()
        steps = x_v[t0 : t0 + n].reshape(n * NS, NP)
        halves += jnp.dot(table[:, t0 * NS : (t0 + n) * NS], steps, preferred_element_type=F32)
    spectrum = (halves[:128] + halves[128:]).astype(BF)
    real, imag = spectrum[:64], spectrum[64:]
    for block in range(2):
        spectra[qj, :, 256 * block : 256 * block + 128] = real[:, 128 * block : 128 * block + 128]
        spectra[qj, :, 256 * block + 128 : 256 * block + 256] = imag[:, 128 * block : 128 * block + 128]
    spectra[qj, :, 512:640] = jnp.concatenate([real[:, 256:320], imag[:, 256:320]], axis=1)

    pl.semaphore_wait(barrier, len(near))
    ag = [
        pltpu.make_async_remote_copy(
            src_ref=spectra.at[qj], dst_ref=spectra.at[qj], send_sem=ag_send.at[d - 1], recv_sem=ag_recv.at[d - 1],
            device_id=(pi, (qj + d) % NQ), device_id_type=MESH,
        )
        for d in range(1, NQ)
    ]
    for copy in ag:
        copy.start()
    for dz in (-NEAR, NEAR):
        pl.semaphore_signal(far, inc=1, device_id=(param_at(0, dz), qj), device_id_type=MESH)

    w_copy.wait()

    def planar_step(f, carry):
        planar(f, w_v, order, w_p)
        return carry

    lax.fori_loop(0, NF // 2, planar_step, 0)
    pl.semaphore_wait(far, 2)
    pl.semaphore_signal(line, inc=1, device_id=(param_at(1, 0), qj), device_id_type=MESH)
    lax.fori_loop(NF // 2, NF, planar_step, 0)
    for copy in ag:
        copy.wait()

    core_copies = []
    even = (lax.broadcasted_iota(jnp.int32, (256, NG), 0) % 8) < 4
    for pair in range(NF // 2):
        part = jnp.concatenate([spectra[q, 16 * pair : 16 * pair + 16, :] for q in range(NQ)], axis=0)
        r0, i0, r1, i1, tail = (part[:, 128 * k : 128 * k + 128] for k in range(5))
        rt, it = tail[:, :64], tail[:, 64:]
        left = jnp.concatenate(
            [
                jnp.concatenate([r0, -i0, r1, -i1, rt, -it], axis=1),
                jnp.concatenate([i0, r0, i1, r1, it, rt], axis=1),
            ],
            axis=0,
        )
        low = jnp.dot(left, w_p[2 * pair], preferred_element_type=F32)
        high = jnp.dot(left, w_p[2 * pair + 1], preferred_element_type=F32)
        both = jnp.where(even, low, high).reshape(2 * NQ, 2, 8, NG)
        own[pair] = both[:, 0]
        give[pair] = both[:, 1].astype(BF)
        copy = pltpu.make_async_remote_copy(
            src_ref=give.at[pair], dst_ref=take.at[pair], send_sem=core_send.at[pair], recv_sem=core_recv.at[pair],
            device_id=(param_at(0, 0, 1), qj), device_id_type=MESH,
        )
        copy.start()
        core_copies.append(copy)

    for pair in range(NF // 2):
        core_copies[pair].wait()
        for k in range(2):
            for q in range(NQ):
                total = own[pair, k * NQ + q] + take[pair, k * NQ + q].astype(F32)
                for half in range(2):
                    spread[q, half, pl.ds(k * 4 + pair, 8, 8), :] = total[:, 128 * half : 128 * half + 128]
    for q in range(NQ):
        for half in range(2):
            send[q, :, :, :, 128 * half : 128 * half + 128] = spread[q, half].reshape(2, 4, 8, 128).astype(BF)

    pl.semaphore_wait(line, 1)
    for dx, dz in owner_offsets():
        px, pz = (xh + dx) % NX, (z + dz + NZ) % NZ
        pltpu.make_async_remote_copy(
            src_ref=send.at[px * 4 + pz // 4, :, pz % 4], dst_ref=recv.at[chip], send_sem=rs_send, recv_sem=rs_recv,
            device_id=((px * NZ + pz) * 2 + core, qj), device_id_type=MESH,
        ).start()

    mine = xh * 4 + z // 4
    at = pl.multiple_of((z % 4) * 8, 8)
    acc0, acc1 = (
        jnp.concatenate([spread[mine, half, pl.ds(at + shift, 8), :] for half in range(2)], axis=1) for shift in (0, 32)
    )
    recv[chip] = jnp.zeros((2, 8, NG), BF)
    group_copy.wait()
    onehot = (lax.broadcasted_iota(jnp.int32, (128, NG), 0) == group_v[...]).astype(F32)

    pltpu.make_async_copy(recv.at[pl.ds(0, 31)], recv.at[pl.ds(0, 31)], rs_recv).wait()
    got = jnp.sum(recv[...].astype(F32), axis=0)
    total = jnp.concatenate([acc0 + got[0], acc1 + got[1]], axis=0)
    acc_out[...] = total
    segs[qj] = lax.dot_general(
        total, onehot, (((1,), (1,)), ((), ())), precision=lax.Precision.HIGHEST, preferred_element_type=F32
    )
    seg = [
        pltpu.make_async_remote_copy(
            src_ref=segs.at[qj], dst_ref=segs.at[qj], send_sem=seg_send.at[d - 1], recv_sem=seg_recv.at[d - 1],
            device_id=(pi, (qj + d) % NQ), device_id_type=MESH,
        )
        for d in range(1, NQ)
    ]
    for copy in seg:
        copy.start()
    pltpu.make_async_copy(recv.at[pl.ds(0, 31)], recv.at[pl.ds(0, 31)], rs_send).wait()
    for copy in seg:
        copy.wait()
    seg_out[...] = jnp.sum(segs[...], axis=0) * math.sqrt(GROUPS / (NG * NQ))


def local(samples, operator_rows, block_start, gauge_group):
    anywhere = pl.BlockSpec(memory_space=pl.ANY)
    in_vmem = pl.BlockSpec(memory_space=pltpu.VMEM)
    dma = pltpu.SemaphoreType.DMA
    acc, seg = pl.pallas_call(
        kernel,
        out_shape=(jax.ShapeDtypeStruct((16, NG), F32), jax.ShapeDtypeStruct((16, 128), F32)),
        in_specs=[anywhere] * 4,
        out_specs=(in_vmem, in_vmem),
        scratch_shapes=[
            pltpu.VMEM((NT, NS, NP), BF),
            pltpu.VMEM((256, NT * NS), BF),
            pltpu.VMEM((2, NF, NT * NS), F32),
            pltpu.VMEM((NF, NP, 2, NG), BF),
            pltpu.VMEM((NF, LANES, NG), BF),
            pltpu.VMEM((2, 256, 256), BF),
            pltpu.VMEM((NQ, 64, LANES), BF),
            pltpu.VMEM((4, 2 * NQ, 8, NG), BF),
            pltpu.VMEM((4, 2 * NQ, 8, NG), BF),
            pltpu.VMEM((4, 2 * NQ, 8, NG), F32),
            pltpu.VMEM((NQ, 2, 64, 128), F32),
            pltpu.VMEM((NQ, 2, 4, 8, NG), BF),
            pltpu.VMEM((NX * NZ, 2, 8, NG), BF),
            pltpu.VMEM((NQ, 16, 128), F32),
            pltpu.SMEM((1,), jnp.int32),
            pltpu.VMEM((1, NG), jnp.int32),
            dma((len(STEPS),)),
            dma,
            dma,
            dma,
            dma((NQ - 1,)),
            dma((NQ - 1,)),
            dma((4,)),
            dma((4,)),
            dma,
            dma,
            dma((NQ - 1,)),
            dma((NQ - 1,)),
            pltpu.SemaphoreType.REGULAR,
            pltpu.SemaphoreType.REGULAR,
        ],
        compiler_params=pltpu.CompilerParams(collective_id=0, has_side_effects=True),
    )(samples.transpose(2, 0, 1), operator_rows, block_start, gauge_group.reshape(1, NG))
    response = acc.reshape(2, 2, 4, NG).transpose(1, 2, 0, 3).reshape(1, 2, NF, NG)
    segment = seg[:, :GROUPS].reshape(2, 2, 4, GROUPS).transpose(1, 2, 0, 3).reshape(1, 2, NF, GROUPS)
    return response, segment


def solution(mesh):
    return jax.shard_map(
        local,
        mesh=mesh,
        in_specs=(P("qoi", "param", None), P(None, "param", None, "qoi"), P(), P("qoi")),
        out_specs=(P("param", None, None, "qoi"), P("param", None, None, None)),
        check_vma=False,
    )
```

```python
import math

import jax
import jax.numpy as jnp
from jax import lax
from jax.experimental import pallas as pl
from jax.experimental.pallas import tpu as pltpu
from jax.sharding import PartitionSpec as P

GROUPS = 16
MESH = pl.DeviceIdType.MESH
BF = jnp.bfloat16
F32 = jnp.float32

NQ = 8
NX = 2
NZ = 16
NF = 8
NT = 420
NS = 8
NP = 320
NG = 256
LANES = 2 * NP
WIDE = 512
TABLE = -(-NT * NS // WIDE) * WIDE
STEPS = ((0, 132), (132, 160), (292, 128))
CUBE = 4
NC = 4
PC = NF // 2 // NC
RB = 4 * PC
scope = jax.named_scope


def rank_of(cube):
    return cube + (cube == 2).astype(jnp.int32) - (cube == 3).astype(jnp.int32)


def owner_offsets():
    return sorted((dz for dz in range(-NZ // 2 + 1, NZ // 2 + 1) if dz), key=lambda dz: (-abs(dz), -dz))


def phase_rows(first, begin, width):
    lane = lax.broadcasted_iota(jnp.int32, (NF, width), 1) + begin
    freq = lax.broadcasted_iota(jnp.int32, (NF, width), 0) + first
    turns = ((lane >> 3) * freq).astype(F32)
    rest = turns - NT * jnp.floor(turns * (1.0 / NT))
    quarter = jnp.floor(rest * (4.0 / NT) + 0.5)
    angle = (rest - (NT // 4) * quarter) * (2.0 * math.pi / NT)
    sq = angle * angle
    sine = angle * (1.0 + sq * (-1.0 / 6 + sq * (1.0 / 120 + sq * (-1.0 / 5040 + sq * (1.0 / 362880)))))
    cosine = 1.0 + sq * (-0.5 + sq * (1.0 / 24 + sq * (-1.0 / 720 + sq * (1.0 / 40320 + sq * (-1.0 / 3628800)))))
    odd = (quarter == 1.0) | (quarter == 3.0)
    scale = 1.0 / math.sqrt(NT)
    cos_all = jnp.where(odd, sine, cosine) * jnp.where((quarter == 1.0) | (quarter == 2.0), -scale, scale)
    sin_all = jnp.where(odd, cosine, sine) * jnp.where((quarter == 2.0) | (quarter == 3.0), scale, -scale)
    return cos_all, sin_all


def fill_table(first, core, rows_ref, table_ref):
    def step(i, carry):
        begin = pl.multiple_of(i * WIDE, WIDE)
        span = pl.ds(begin, WIDE)
        rows_ref[0], rows_ref[1] = phase_rows(first, begin, WIDE)
        sample = lax.broadcasted_iota(jnp.int32, (16, WIDE), 1) % NS
        row = lax.broadcasted_iota(jnp.int32, (16, WIDE), 0)
        side = jnp.where(row < 8, core, 1 - core)
        hit = sample == ((row % 8) // 2) * 2 + side
        upper = row % 2 == 1
        for part in range(2):
            for pair in range(NF // 2):
                low = jnp.broadcast_to(rows_ref[part, 2 * pair : 2 * pair + 1], (16, WIDE))
                high = jnp.broadcast_to(rows_ref[part, 2 * pair + 1 : 2 * pair + 2], (16, WIDE))
                value = jnp.where(hit, jnp.where(upper, high, low), 0.0)
                rounded = value.astype(BF)
                at = part * 64 + pair * 16
                table_ref[at : at + 16, span] = rounded
                table_ref[128 + at : 144 + at, span] = (value - rounded.astype(F32)).astype(BF)
        return carry

    lax.fori_loop(0, TABLE // WIDE, step, 0)


def diagonal(shape):
    return lax.broadcasted_iota(jnp.int32, shape, 2) // GROUPS == lax.broadcasted_iota(jnp.int32, shape, 1)


def planar(f, w_ref, order_ref, out_ref):
    for begin in range(0, NP, 128):
        count = min(128, NP - begin)
        rows = w_ref[f, begin : begin + count].reshape(2 * count, NG)
        order = order_ref[0] if count == 128 else order_ref[1, : 2 * count, : 2 * count]
        out_ref[f, 2 * begin : 2 * (begin + count)] = jnp.dot(order, rows, preferred_element_type=F32).astype(BF)


def kernel(
    x_hbm, w_hbm, first_ref, group_hbm, acc_out, seg_out,
    x_v, table, rows, w_v, w_p, order, spectra, give, take, own, x_give, x_take, kept, spread, send, recv, segs, group_v,
    x_sem, w_sem, group_sem, ag_send, ag_recv, core_send, core_recv, x_send, x_recv, rs_send, rs_recv, seg_send, seg_recv,
    around, above,
):
    pi, qj = lax.axis_index("param"), lax.axis_index("qoi")
    core, chip = pi % 2, pi // 2
    xh, z = chip // NZ, chip % NZ

    def param_at(dx, dz, dc=0):
        return (((xh + dx) % NX) * NZ + (z + dz + NZ) % NZ) * 2 + (core + dc) % 2

    with scope("begin"):
        x_copies = [
            pltpu.make_async_copy(x_hbm.at[pl.ds(t0, n)], x_v.at[pl.ds(t0, n)], x_sem.at[i])
            for i, (t0, n) in enumerate(STEPS)
        ]
        w_copy = pltpu.make_async_copy(w_hbm, w_v, w_sem)
        group_copy = pltpu.make_async_copy(group_hbm, group_v, group_sem)
        for copy in x_copies:
            copy.start()

    place, cube = z % CUBE, z // CUBE
    rank = rank_of(cube)
    plane = [(param_at(1, 0), qj), (param_at(0, 0, 1), qj)] + [(pi, (qj + d) % NQ) for d in range(1, NQ)]
    within = [(((xh * NZ) + cube * CUBE + (place + d) % CUBE) * 2 + core, qj) for d in range(1, CUBE)]
    others = [((cube + d) % (NZ // CUBE), (param_at(0, CUBE * d), qj)) for d in range(1, NZ // CUBE)]
    with scope("signals"):
        barrier = pltpu.get_barrier_semaphore()
        for peer in plane + within:
            pl.semaphore_signal(barrier, inc=1, device_id=peer, device_id_type=MESH)
        for other, peer in others:
            @pl.when(rank_of(other) > rank)
            def _():
                pl.semaphore_signal(barrier, inc=1, device_id=peer, device_id_type=MESH)

    with scope("table"):
        fill_table(first_ref[0], core, rows, table)
        w_copy.start()
        group_copy.start()

    with scope("dft"):
        halves = None
        for copy, (t0, n) in zip(x_copies, STEPS):
            with scope("xw"):
                copy.wait()
            steps = x_v[t0 : t0 + n].reshape(n * NS, NP)
            term = jnp.dot(table[:, t0 * NS : (t0 + n) * NS], steps, preferred_element_type=F32)
            halves = term if halves is None else halves + term
        spectrum = (halves[:128] + halves[128:]).astype(BF)
        real, imag = spectrum[:64], spectrum[64:]
        for block in range(2):
            spectra[qj, :, 256 * block : 256 * block + 128] = real[:, 128 * block : 128 * block + 128]
            spectra[qj, :, 256 * block + 128 : 256 * block + 256] = imag[:, 128 * block : 128 * block + 128]
        spectra[qj, :, 512:640] = jnp.concatenate([real[:, 256:320], imag[:, 256:320]], axis=1)

    def ag_copy(c, d):
        block = spectra.at[qj, pl.ds(pl.multiple_of(16 * PC * c, 16 * PC), 16 * PC)]
        return pltpu.make_async_remote_copy(
            src_ref=block, dst_ref=block, send_sem=ag_send, recv_sem=ag_recv.at[c],
            device_id=(pi, (qj + d) % NQ), device_id_type=MESH,
        )

    def ag_all(c):
        return spectra.at[pl.ds(0, NQ - 1), pl.ds(pl.multiple_of(16 * PC * c, 16 * PC), 16 * PC)]

    with scope("near"):
        pl.semaphore_wait(barrier, len(plane) + len(within) + rank)
    with scope("ag_start"):
        def ag_step(c, carry):
            for d in range(1, NQ):
                ag_copy(c, d).start()
            return carry

        lax.fori_loop(0, NC, ag_step, 0)
        for peer in within:
            pl.semaphore_signal(around, inc=1, device_id=peer, device_id_type=MESH)

    def planar_step(f, carry):
        planar(f, w_v, order, w_p)
        return carry

    with scope("planar0"):
        big = lax.broadcasted_iota(jnp.int32, (256, 256), 0)
        col = lax.broadcasted_iota(jnp.int32, (256, 256), 1)
        order[0] = jnp.where(col == (big % 128) * 2 + big // 128, 1.0, 0.0).astype(BF)
        order[1] = jnp.where(col == (big % 64) * 2 + (big // 64) % 2, 1.0, 0.0).astype(BF)
        w_copy.wait()
        lax.fori_loop(0, NF // 2, planar_step, 0)
    with scope("around"):
        pl.semaphore_wait(around, len(within))
        for other, peer in others:
            @pl.when(rank_of(other) < rank)
            def _():
                pl.semaphore_signal(above, inc=1, device_id=peer, device_id_type=MESH)

    with scope("planar1"):
        lax.fori_loop(NF // 2, NF, planar_step, 0)
        group_copy.wait()

    even = (lax.broadcasted_iota(jnp.int32, (256, NG), 0) % 2) == 0

    def core_copy(pair):
        return pltpu.make_async_remote_copy(
            src_ref=give.at[pair], dst_ref=take.at[pair], send_sem=core_send, recv_sem=core_recv.at[pair],
            device_id=(param_at(0, 0, 1), qj), device_id_type=MESH,
        )

    def product(pair):
        at = pl.multiple_of(16 * pair, 16)
        part = jnp.concatenate([spectra[q, pl.ds(at, 16), :] for q in range(NQ)], axis=0)
        r0, i0, r1, i1, tail = (part[:, 128 * k : 128 * k + 128] for k in range(5))
        rt, it = tail[:, :64], tail[:, 64:]
        left = jnp.concatenate(
            [
                jnp.concatenate([r0, -i0, r1, -i1, rt, -it], axis=1),
                jnp.concatenate([i0, r0, i1, r1, it, rt], axis=1),
            ],
            axis=0,
        )
        low = jnp.dot(left, w_p[2 * pair], preferred_element_type=F32)
        high = jnp.dot(left, w_p[2 * pair + 1], preferred_element_type=F32)
        both = jnp.where(even, low, high).reshape(2 * NQ, 2, 8, NG)
        give[pair] = both[:, 1].astype(BF)
        core_copy(pair).start()
        own[pair] = both[:, 0]

    half_q = NQ // NX

    def x_copy(c):
        return pltpu.make_async_remote_copy(
            src_ref=x_give.at[c], dst_ref=x_take.at[c], send_sem=x_send, recv_sem=x_recv.at[c],
            device_id=(param_at(1, 0), qj), device_id_type=MESH,
        )

    def across(c):
        for p in range(PC):
            pair = c * PC + p
            with scope("core_wait"):
                core_copy(pair).wait_recv()
            for k in range(2):
                at = k * NQ + (1 - xh) * half_q
                x_give[c, p, k] = (own[pair, pl.ds(at, half_q)] + take[pair, pl.ds(at, half_q)].astype(F32)).astype(BF)
        x_copy(c).start()
        for p in range(PC):
            pair = c * PC + p
            for k in range(2):
                at = k * NQ + xh * half_q
                kept[c, p, k] = own[pair, pl.ds(at, half_q)] + take[pair, pl.ds(at, half_q)].astype(F32)

    def sums(c):
        with scope("x_wait"):
            x_copy(c).wait_recv()
        for q in range(half_q):
            for p in range(PC):
                for k in range(2):
                    total = kept[c, p, k, q] + x_take[c, p, k, q].astype(F32)
                    for half in range(2):
                        spread[c, q, half, pl.ds(k * PC + p, 8, 2 * PC), :] = total[:, 128 * half : 128 * half + 128]
        for q in range(half_q):
            for half in range(2):
                send[c, q, :, :, 128 * half : 128 * half + 128] = spread[c, q, half].reshape(4, RB, 128).astype(BF)

    def give_out(c, later):
        for dz in owner_offsets():
            pz = (z + dz + NZ) % NZ
            known = rank_of(pz // CUBE) <= rank

            @pl.when(jnp.logical_not(known) if later else known)
            def _():
                pltpu.make_async_remote_copy(
                    src_ref=send.at[c, pz // 4, pz % 4], dst_ref=recv.at[c, z],
                    send_sem=rs_send, recv_sem=rs_recv.at[c],
                    device_id=(param_at(0, dz), qj), device_id_type=MESH,
                ).start()
        if not later:
            recv[c, z] = jnp.zeros((RB, NG), BF)

    for c in range(NC):
        with scope(f"ag_wait{c}"):
            pltpu.make_async_copy(ag_all(c), ag_all(c), ag_recv.at[c]).wait()
        with scope(f"products{c}"):
            for p in range(PC):
                product(c * PC + p)
        if c > 0:
            with scope(f"across{c - 1}"):
                across(c - 1)
    with scope(f"across{NC - 1}"):
        across(NC - 1)
    for c in range(NC):
        with scope(f"sums{c}"):
            sums(c)
        with scope(f"rs_start{c}"):
            give_out(c, False)

    @pl.when(rank < NZ // CUBE - 1)
    def _():
        with scope("above"):
            pl.semaphore_wait(above, NZ // CUBE - 1 - rank)
        with scope("rs_later"):
            for c in range(NC):
                give_out(c, True)

    mine = z // 4
    onehot = (lax.broadcasted_iota(jnp.int32, (128, NG), 0) % GROUPS == group_v[...]).astype(F32)
    for c in range(NC):
        with scope(f"rs_wait{c}"):
            whole = recv.at[c, pl.ds(0, NZ - 1)]
            pltpu.make_async_copy(whole, whole, rs_recv.at[c]).wait()
        with scope(f"final{c}"):
            at = pl.multiple_of((z % 4) * RB, RB)
            here = jnp.concatenate([spread[c, mine, half, pl.ds(at, RB), :] for half in range(2)], axis=1)
            total = here + jnp.sum(recv[c].astype(F32), axis=0)
            for f2 in range(2):
                for k in range(2):
                    for p in range(PC):
                        row = (f2 * 2 + k) * PC + p
                        acc_out[k, (c * PC + p) * 2 + f2 : (c * PC + p) * 2 + f2 + 1, :] = total[row : row + 1]
    with scope("segment"):
        grouped = lax.dot_general(
            acc_out[...].reshape(16, NG), onehot, (((1,), (1,)), ((), ())),
            precision=lax.Precision.HIGHEST, preferred_element_type=F32,
        )
        segs[qj] = jnp.sum(jnp.where(diagonal((2, NF, 128)), grouped.reshape(2, NF, 128), 0.0), axis=1)
        seg = [
            pltpu.make_async_remote_copy(
                src_ref=segs.at[qj], dst_ref=segs.at[qj], send_sem=seg_send, recv_sem=seg_recv,
                device_id=(pi, (qj + d) % NQ), device_id_type=MESH,
            )
            for d in range(1, NQ)
        ]
        for copy in seg:
            copy.start()
    with scope("send_waits"):
        whole = recv.at[:, pl.ds(0, NZ - 1)]
        pltpu.make_async_copy(whole, whole, rs_send).wait()
        sent = spectra.at[pl.ds(0, NQ - 1)]
        pltpu.make_async_copy(sent, sent, ag_send).wait()
        pltpu.make_async_copy(give, give, core_send).wait()
        pltpu.make_async_copy(x_give, x_give, x_send).wait()
    with scope("seg_wait"):
        pltpu.make_async_copy(segs.at[pl.ds(0, NQ - 1)], segs.at[pl.ds(0, NQ - 1)], seg_recv).wait()
        pltpu.make_async_copy(segs.at[pl.ds(0, NQ - 1)], segs.at[pl.ds(0, NQ - 1)], seg_send).wait()
    seg_out[...] = jnp.sum(segs[...], axis=0) * math.sqrt(GROUPS / (NG * NQ))


def finish(acc_ref, seg_ref, response_ref, segment_ref):
    response_ref[0] = acc_ref[...]
    for f in range(NF):
        segment_ref[0, :, f, :] = seg_ref[:, GROUPS * f : GROUPS * (f + 1)]


def local(samples, operator_rows, block_start, gauge_group):
    in_hbm = pl.BlockSpec(memory_space=pltpu.HBM)
    in_vmem = pl.BlockSpec(memory_space=pltpu.VMEM)
    dma = pltpu.SemaphoreType.DMA
    acc, seg = pl.pallas_call(
        kernel,
        out_shape=(pltpu.VMEM((2, NF, NG), F32), pltpu.VMEM((2, 128), F32)),
        in_specs=[in_hbm, in_hbm, pl.BlockSpec(memory_space=pltpu.SMEM), in_hbm],
        out_specs=(in_vmem, in_vmem),
        scratch_shapes=[
            pltpu.VMEM((NT, NS, NP), BF),
            pltpu.VMEM((256, TABLE), BF),
            pltpu.VMEM((2, NF, WIDE), F32),
            pltpu.VMEM((NF, NP, 2, NG), BF),
            pltpu.VMEM((NF, LANES, NG), BF),
            pltpu.VMEM((2, 256, 256), BF),
            pltpu.VMEM((NQ, 64, LANES), BF),
            pltpu.VMEM((4, 2 * NQ, 8, NG), BF),
            pltpu.VMEM((4, 2 * NQ, 8, NG), BF),
            pltpu.VMEM((4, 2 * NQ, 8, NG), F32),
            pltpu.VMEM((NC, PC, 2, NQ // NX, 8, NG), BF),
            pltpu.VMEM((NC, PC, 2, NQ // NX, 8, NG), BF),
            pltpu.VMEM((NC, PC, 2, NQ // NX, 8, NG), F32),
            pltpu.VMEM((NC, NQ // NX, 2, 8 * 2 * PC, 128), F32),
            pltpu.VMEM((NC, NQ // NX, 4, RB, NG), BF),
            pltpu.VMEM((NC, NZ, RB, NG), BF),
            pltpu.VMEM((NQ, 2, 128), F32),
            pltpu.VMEM((1, NG), jnp.int32),
            dma((len(STEPS),)),
            dma,
            dma,
            dma,
            dma((NC,)),
            dma,
            dma((4,)),
            dma,
            dma((NC,)),
            dma,
            dma((NC,)),
            dma,
            dma,
            pltpu.SemaphoreType.REGULAR,
            pltpu.SemaphoreType.REGULAR,
        ],
        compiler_params=pltpu.CompilerParams(collective_id=0, has_side_effects=True),
    )(samples.transpose(2, 0, 1), operator_rows, block_start, gauge_group.reshape(1, NG))
    return pl.pallas_call(
        finish,
        out_shape=(jax.ShapeDtypeStruct((1, 2, NF, NG), F32), jax.ShapeDtypeStruct((1, 2, NF, GROUPS), F32)),
        in_specs=[in_vmem] * 2,
        out_specs=(in_vmem, in_vmem),
    )(pltpu.with_memory_space_constraint(acc, pltpu.VMEM), pltpu.with_memory_space_constraint(seg, pltpu.VMEM))


def solution(mesh):
    return jax.shard_map(
        local,
        mesh=mesh,
        in_specs=(P("qoi", "param", None), P(None, "param", None, "qoi"), P(), P("qoi")),
        out_specs=(P("param", None, None, "qoi"), P("param", None, None, None)),
        check_vma=False,
    )
```

```python
import math

import jax
import jax.numpy as jnp
from jax import lax
from jax.experimental import pallas as pl
from jax.experimental.pallas import tpu as pltpu
from jax.sharding import PartitionSpec as P

GROUPS = 16
MESH = pl.DeviceIdType.MESH
BF = jnp.bfloat16
F32 = jnp.float32

NQ = 8
NY = 4
NX = 2
NZ = 16
NF = 8
NT = 420
NS = 8
NP = 320
NG = 256
LANES = 2 * NP
WIDE = 512
TABLE = -(-NT * NS // WIDE) * WIDE
STEPS = ((0, 68), (68, 128), (196, 128), (324, 96))
CUBE = 4
NC = 4
PC = NF // 2 // NC
RB = 4 * PC
ROUTES = "xyxy"
STAGED = 3
SLOTS = STAGED * NZ + (NC - STAGED) * NX * NZ
ARRIVALS = STAGED * (NZ - 1) + (NC - STAGED) * (NX * NZ - 1)
scope = jax.named_scope


def rank_of(cube):
    return cube + (cube == 2).astype(jnp.int32) - (cube == 3).astype(jnp.int32)


def owner_offsets(lines):
    pairs = [(dx, dz) for dx in range(lines) for dz in range(-NZ // 2 + 1, NZ // 2 + 1) if (dx, dz) != (0, 0)]
    return sorted(pairs, key=lambda pair: (-(abs(pair[1]) + 2 * pair[0]), -pair[1]))


def phase_rows(first, begin, width):
    lane = lax.broadcasted_iota(jnp.int32, (NF, width), 1) + begin
    freq = lax.broadcasted_iota(jnp.int32, (NF, width), 0) + first
    turns = ((lane >> 3) * freq).astype(F32)
    rest = turns - NT * jnp.floor(turns * (1.0 / NT))
    quarter = jnp.floor(rest * (4.0 / NT) + 0.5)
    angle = (rest - (NT // 4) * quarter) * (2.0 * math.pi / NT)
    sq = angle * angle
    sine = angle * (1.0 + sq * (-1.0 / 6 + sq * (1.0 / 120 + sq * (-1.0 / 5040 + sq * (1.0 / 362880)))))
    cosine = 1.0 + sq * (-0.5 + sq * (1.0 / 24 + sq * (-1.0 / 720 + sq * (1.0 / 40320 + sq * (-1.0 / 3628800)))))
    odd = (quarter == 1.0) | (quarter == 3.0)
    scale = 1.0 / math.sqrt(NT)
    cos_all = jnp.where(odd, sine, cosine) * jnp.where((quarter == 1.0) | (quarter == 2.0), -scale, scale)
    sin_all = jnp.where(odd, cosine, sine) * jnp.where((quarter == 2.0) | (quarter == 3.0), scale, -scale)
    return cos_all, sin_all


def fill_table(first, core, rows_ref, table_ref):
    def step(i, carry):
        begin = pl.multiple_of(i * WIDE, WIDE)
        span = pl.ds(begin, WIDE)
        rows_ref[0], rows_ref[1] = phase_rows(first, begin, WIDE)
        sample = lax.broadcasted_iota(jnp.int32, (16, WIDE), 1) % NS
        row = lax.broadcasted_iota(jnp.int32, (16, WIDE), 0)
        side = jnp.where(row < 8, core, 1 - core)
        hit = sample == ((row % 8) // 2) * 2 + side
        upper = row % 2 == 1
        for part in range(2):
            for pair in range(NF // 2):
                low = jnp.broadcast_to(rows_ref[part, 2 * pair : 2 * pair + 1], (16, WIDE))
                high = jnp.broadcast_to(rows_ref[part, 2 * pair + 1 : 2 * pair + 2], (16, WIDE))
                value = jnp.where(hit, jnp.where(upper, high, low), 0.0)
                rounded = value.astype(BF)
                at = part * 64 + pair * 16
                table_ref[at : at + 16, span] = rounded
                table_ref[128 + at : 144 + at, span] = (value - rounded.astype(F32)).astype(BF)
        return carry

    lax.fori_loop(0, TABLE // WIDE, step, 0)


def diagonal(shape):
    return lax.broadcasted_iota(jnp.int32, shape, 2) // GROUPS == lax.broadcasted_iota(jnp.int32, shape, 1)


def planar(f, w_ref, order_ref, out_ref):
    for begin in range(0, NP, 128):
        count = min(128, NP - begin)
        rows = w_ref[f, begin : begin + count].reshape(2 * count, NG)
        order = order_ref[0] if count == 128 else order_ref[1, : 2 * count, : 2 * count]
        out_ref[f, 2 * begin : 2 * (begin + count)] = jnp.dot(order, rows, preferred_element_type=F32).astype(BF)


def kernel(
    x_hbm, w_hbm, first_ref, group_hbm, acc_out, seg_out,
    x_v, table, rows, w_v, w_p, order, spectra, give, take, own, x_give, x_take, kept, spread, send, recv, segs, group_v,
    x_sem, w_sem, group_sem, ag_send, ag_first, ag_recv, core_send, core_recv, x_send, x_recv, rs_send, rs_recv, seg_send, seg_recv,
    around, line, above,
):
    pi, qj = lax.axis_index("param"), lax.axis_index("qoi")
    core, chip = pi % 2, pi // 2
    xh, z = chip // NZ, chip % NZ

    def param_at(dx, dz, dc=0):
        return (((xh + dx) % NX) * NZ + (z + dz + NZ) % NZ) * 2 + (core + dc) % 2

    with scope("begin"):
        x_copies = [
            pltpu.make_async_copy(x_hbm.at[pl.ds(t0, n)], x_v.at[pl.ds(t0, n)], x_sem.at[i])
            for i, (t0, n) in enumerate(STEPS)
        ]
        w_copy = pltpu.make_async_copy(w_hbm, w_v, w_sem)
        group_copy = pltpu.make_async_copy(group_hbm, group_v, group_sem)
        for copy in x_copies:
            copy.start()

    place, cube = z % CUBE, z // CUBE
    rank = rank_of(cube)
    plane = [(param_at(1, 0), qj), (param_at(0, 0, 1), qj)] + [(pi, (qj + d) % NQ) for d in range(1, NQ)]
    within = [(((xh * NZ) + cube * CUBE + (place + d) % CUBE) * 2 + core, qj) for d in range(1, CUBE)]
    others = [((cube + d) % (NZ // CUBE), (param_at(0, CUBE * d), qj)) for d in range(1, NZ // CUBE)]
    with scope("signals"):
        barrier = pltpu.get_barrier_semaphore()
        for peer in plane + within:
            pl.semaphore_signal(barrier, inc=1, device_id=peer, device_id_type=MESH)
        for other, peer in others:
            @pl.when(rank_of(other) > rank)
            def _():
                pl.semaphore_signal(barrier, inc=1, device_id=peer, device_id_type=MESH)

    with scope("table"):
        fill_table(first_ref[0], core, rows, table)
        w_copy.start()
        group_copy.start()

    with scope("dft"):
        halves = None
        for copy, (t0, n) in zip(x_copies, STEPS):
            copy.wait()
            steps = x_v[t0 : t0 + n].reshape(n * NS, NP)
            term = jnp.dot(table[:, t0 * NS : (t0 + n) * NS], steps, preferred_element_type=F32)
            halves = term if halves is None else halves + term
        spectrum = (halves[:128] + halves[128:]).astype(BF)
        real, imag = spectrum[:64], spectrum[64:]
        for block in range(2):
            spectra[qj, :, 256 * block : 256 * block + 128] = real[:, 128 * block : 128 * block + 128]
            spectra[qj, :, 256 * block + 128 : 256 * block + 256] = imag[:, 128 * block : 128 * block + 128]
        spectra[qj, :, 512:640] = jnp.concatenate([real[:, 256:320], imag[:, 256:320]], axis=1)

    xl, y = qj // NY, qj % NY
    beside = (1 - xl) * NY + y
    along = [xl * NY + (y + d) % NY for d in range(1, NY)]

    def chunk_of(q, c):
        return spectra.at[q, pl.ds(16 * PC * c, 16 * PC)]

    def ag_copy(q, c, peer, sem):
        return pltpu.make_async_remote_copy(
            src_ref=chunk_of(q, c), dst_ref=chunk_of(q, c), send_sem=ag_send, recv_sem=sem.at[c],
            device_id=(pi, peer), device_id_type=MESH,
        )

    def await_blocks(count, c, sem):
        blocks = spectra.at[pl.ds(0, count), pl.ds(16 * PC * c, 16 * PC)]
        pltpu.make_async_copy(blocks, blocks, sem.at[c]).wait()

    def hand_on(c):
        if ROUTES[c] == "x":
            await_blocks(1, c, ag_first)
            for peer in along:
                ag_copy(beside, c, peer, ag_recv).start()
        if ROUTES[c] == "y":
            await_blocks(NY - 1, c, ag_first)
            for q in along:
                ag_copy(q, c, beside, ag_recv).start()

    def ag_wait(c):
        await_blocks({"d": NQ - 1, "x": 2 * (NY - 1), "y": NY}[ROUTES[c]], c, ag_recv)

    with scope("near"):
        pl.semaphore_wait(barrier, len(plane) + len(within) + rank)
    with scope("ag_start"):
        for c in sorted(range(NC), key=lambda c: ROUTES[c] != "x"):
            ag_copy(qj, c, beside, ag_first if ROUTES[c] == "x" else ag_recv).start()
        for c in sorted(range(NC), key=lambda c: ROUTES[c] == "x"):
            for peer in along:
                ag_copy(qj, c, peer, ag_first if ROUTES[c] == "y" else ag_recv).start()
            if ROUTES[c] == "d":
                for d in range(1, NY):
                    ag_copy(qj, c, (1 - xl) * NY + (y + d) % NY, ag_recv).start()
        for peer in within:
            pl.semaphore_signal(around, inc=1, device_id=peer, device_id_type=MESH)

    def planar_step(f, carry):
        planar(f, w_v, order, w_p)
        return carry

    with scope("planar0"):
        big = lax.broadcasted_iota(jnp.int32, (256, 256), 0)
        col = lax.broadcasted_iota(jnp.int32, (256, 256), 1)
        order[0] = jnp.where(col == (big % 128) * 2 + big // 128, 1.0, 0.0).astype(BF)
        order[1] = jnp.where(col == (big % 64) * 2 + (big // 64) % 2, 1.0, 0.0).astype(BF)
        w_copy.wait()
        lax.fori_loop(0, NF // 2, planar_step, 0)
    with scope("around"):
        pl.semaphore_wait(around, len(within))
        pl.semaphore_signal(line, inc=1, device_id=(param_at(1, 0), qj), device_id_type=MESH)
    with scope("hand0"):
        for c in range(NC):
            if ROUTES[c] == "x":
                hand_on(c)
    with scope("planar1"):
        lax.fori_loop(NF // 2, NF * 3 // 4, planar_step, 0)
    with scope("hand1"):
        hand_on(1)
    with scope("planar2"):
        lax.fori_loop(NF * 3 // 4, NF, planar_step, 0)
        group_copy.wait()
    with scope("hand3"):
        hand_on(3)

    with scope("line"):
        pl.semaphore_wait(line, 1)
        for other, peer in others:
            @pl.when(rank_of(other) < rank)
            def _():
                pl.semaphore_signal(above, inc=1, device_id=peer, device_id_type=MESH)

    even = (lax.broadcasted_iota(jnp.int32, (256, NG), 0) % 2) == 0

    def core_copy(pair):
        return pltpu.make_async_remote_copy(
            src_ref=give.at[pair], dst_ref=take.at[pair], send_sem=core_send, recv_sem=core_recv.at[pair],
            device_id=(param_at(0, 0, 1), qj), device_id_type=MESH,
        )

    def product(pair):
        at = pl.multiple_of(16 * pair, 16)
        part = jnp.concatenate([spectra[q, pl.ds(at, 16), :] for q in range(NQ)], axis=0)
        r0, i0, r1, i1, tail = (part[:, 128 * k : 128 * k + 128] for k in range(5))
        rt, it = tail[:, :64], tail[:, 64:]
        left = jnp.concatenate(
            [
                jnp.concatenate([r0, -i0, r1, -i1, rt, -it], axis=1),
                jnp.concatenate([i0, r0, i1, r1, it, rt], axis=1),
            ],
            axis=0,
        )
        low = jnp.dot(left, w_p[2 * pair], preferred_element_type=F32)
        high = jnp.dot(left, w_p[2 * pair + 1], preferred_element_type=F32)
        both = jnp.where(even, low, high).reshape(2 * NQ, 2, 8, NG)
        give[pair] = both[:, 1].astype(BF)
        core_copy(pair).start()
        own[pair] = both[:, 0]

    half_q = NQ // NX

    def x_copy(c):
        return pltpu.make_async_remote_copy(
            src_ref=x_give.at[c], dst_ref=x_take.at[c], send_sem=x_send, recv_sem=x_recv.at[c],
            device_id=(param_at(1, 0), qj), device_id_type=MESH,
        )

    def across(c):
        for p in range(PC):
            pair = c * PC + p
            with scope("core_wait"):
                core_copy(pair).wait_recv()
            for k in range(2):
                at = k * NQ + (1 - xh) * half_q
                x_give[c, p, k] = (own[pair, pl.ds(at, half_q)] + take[pair, pl.ds(at, half_q)].astype(F32)).astype(BF)
        x_copy(c).start()
        for p in range(PC):
            pair = c * PC + p
            for k in range(2):
                at = k * NQ + xh * half_q
                kept[c, p, k] = own[pair, pl.ds(at, half_q)] + take[pair, pl.ds(at, half_q)].astype(F32)

    def lay(c, first, count, total):
        for q in range(count):
            for p in range(PC):
                for k in range(2):
                    value = total(p, k, q)
                    for half in range(2):
                        spread[first + q, half, pl.ds(k * PC + p, 8, 2 * PC), :] = value[:, 128 * half : 128 * half + 128]
        for q in range(count):
            for half in range(2):
                send[first + q, :, :, 128 * half : 128 * half + 128] = (
                    spread[first + q, half].reshape(4, RB, 128).astype(BF)
                )

    def sums(c):
        if c < STAGED:
            with scope("x_wait"):
                x_copy(c).wait_recv()
            lay(c, c * half_q, half_q, lambda p, k, q: kept[c, p, k, q] + x_take[c, p, k, q].astype(F32))
        else:
            for p in range(PC):
                core_copy(c * PC + p).wait_recv()
            lay(
                c, STAGED * half_q + (c - STAGED) * NQ, NQ,
                lambda p, k, q: own[c * PC + p, k * NQ + q] + take[c * PC + p, k * NQ + q].astype(F32),
            )

    def place_of(c, px, pz):
        return (c * half_q if c < STAGED else STAGED * half_q + (c - STAGED) * NQ + px * half_q) + pz // 4

    def slot_of(c):
        return c * NZ + z if c < STAGED else STAGED * NZ + (c - STAGED) * NX * NZ + chip

    def give_out(c, later):
        for dx, dz in owner_offsets(1 if c < STAGED else NX):
            px, pz = (xh + dx) % NX, (z + dz + NZ) % NZ
            known = rank_of(pz // CUBE) <= rank

            @pl.when(jnp.logical_not(known) if later else known)
            def _():
                pltpu.make_async_remote_copy(
                    src_ref=send.at[place_of(c, px, pz), pz % 4], dst_ref=recv.at[slot_of(c)],
                    send_sem=rs_send, recv_sem=rs_recv,
                    device_id=(param_at(dx, dz), qj), device_id_type=MESH,
                ).start()
        if not later:
            recv[slot_of(c)] = jnp.zeros((RB, NG), BF)

    def products(c):
        with scope(f"ag_wait{c}"):
            ag_wait(c)
        with scope(f"products{c}"):
            for p in range(PC):
                product(c * PC + p)

    def leave(c):
        with scope(f"sums{c}"):
            sums(c)
        with scope(f"rs_start{c}"):
            give_out(c, False)

    for c in range(NC):
        products(c)
        if 2 <= c < STAGED + 2:
            with scope(f"across{c - 2}"):
                across(c - 2)
        elif c - 2 >= STAGED:
            leave(c - 2)
    for c in range(max(NC - 2, 0), NC):
        if c < STAGED:
            with scope(f"across{c}"):
                across(c)
        else:
            leave(c)
    for c in range(STAGED):
        leave(c)

    @pl.when(rank < NZ // CUBE - 1)
    def _():
        with scope("above"):
            pl.semaphore_wait(above, NZ // CUBE - 1 - rank)
        with scope("rs_later"):
            for c in range(NC):
                give_out(c, True)

    onehot = (lax.broadcasted_iota(jnp.int32, (128, NG), 0) % GROUPS == group_v[...]).astype(F32).astype(BF)
    with scope("rs_wait"):
        whole = recv.at[pl.ds(0, ARRIVALS)]
        pltpu.make_async_copy(whole, whole, rs_recv).wait()
    for c in range(NC):
        with scope(f"final{c}"):
            at = pl.multiple_of((z % 4) * RB, RB)
            mine = place_of(c, xh, z)
            here = jnp.concatenate([spread[mine, half, pl.ds(at, RB), :] for half in range(2)], axis=1)
            if c < STAGED:
                slots = slice(c * NZ, (c + 1) * NZ)
            else:
                slots = slice(STAGED * NZ + (c - STAGED) * NX * NZ, STAGED * NZ + (c - STAGED + 1) * NX * NZ)
            total = here + jnp.sum(recv[slots].astype(F32), axis=0)
            for f2 in range(2):
                for k in range(2):
                    for p in range(PC):
                        row = (f2 * 2 + k) * PC + p
                        acc_out[k, (c * PC + p) * 2 + f2 : (c * PC + p) * 2 + f2 + 1, :] = total[row : row + 1]
    with scope("segment"):
        sums_all = acc_out[...].reshape(16, NG)
        top = sums_all.astype(BF)
        rest = sums_all - top.astype(F32)
        middle = rest.astype(BF)
        low = (rest - middle.astype(F32)).astype(BF)
        terms = lax.dot_general(
            jnp.concatenate([top, middle, low], axis=0), onehot, (((1,), (1,)), ((), ())), preferred_element_type=F32
        )
        grouped = terms[:16] + terms[16:32] + terms[32:]
        segs[qj] = jnp.sum(jnp.where(diagonal((2, NF, 128)), grouped.reshape(2, NF, 128), 0.0), axis=1)
        seg = [
            pltpu.make_async_remote_copy(
                src_ref=segs.at[qj], dst_ref=segs.at[qj], send_sem=seg_send, recv_sem=seg_recv,
                device_id=(pi, (qj + d) % NQ), device_id_type=MESH,
            )
            for d in range(1, NQ)
        ]
        for copy in seg:
            copy.start()
    with scope("send_waits"):
        whole = recv.at[pl.ds(0, ARRIVALS)]
        pltpu.make_async_copy(whole, whole, rs_send).wait()
        sent = spectra.at[pl.ds(0, NQ - 1)]
        pltpu.make_async_copy(sent, sent, ag_send).wait()
        pltpu.make_async_copy(give, give, core_send).wait()
        pltpu.make_async_copy(x_give, x_give, x_send).wait()
    with scope("seg_wait"):
        pltpu.make_async_copy(segs.at[pl.ds(0, NQ - 1)], segs.at[pl.ds(0, NQ - 1)], seg_recv).wait()
        pltpu.make_async_copy(segs.at[pl.ds(0, NQ - 1)], segs.at[pl.ds(0, NQ - 1)], seg_send).wait()
    seg_out[...] = jnp.sum(segs[...], axis=0) * math.sqrt(GROUPS / (NG * NQ))


def finish(acc_ref, seg_ref, response_ref, segment_ref):
    response_ref[0] = acc_ref[...]
    for f in range(NF):
        segment_ref[0, :, f, :] = seg_ref[:, GROUPS * f : GROUPS * (f + 1)]


def local(samples, operator_rows, block_start, gauge_group):
    in_hbm = pl.BlockSpec(memory_space=pltpu.HBM)
    in_vmem = pl.BlockSpec(memory_space=pltpu.VMEM)
    dma = pltpu.SemaphoreType.DMA
    acc, seg = pl.pallas_call(
        kernel,
        out_shape=(pltpu.VMEM((2, NF, NG), F32), pltpu.VMEM((2, 128), F32)),
        in_specs=[in_hbm, in_hbm, pl.BlockSpec(memory_space=pltpu.SMEM), in_hbm],
        out_specs=(in_vmem, in_vmem),
        scratch_shapes=[
            pltpu.VMEM((NT, NS, NP), BF),
            pltpu.VMEM((256, TABLE), BF),
            pltpu.VMEM((2, NF, WIDE), F32),
            pltpu.VMEM((NF, NP, 2, NG), BF),
            pltpu.VMEM((NF, LANES, NG), BF),
            pltpu.VMEM((2, 256, 256), BF),
            pltpu.VMEM((NQ, 64, LANES), BF),
            pltpu.VMEM((4, 2 * NQ, 8, NG), BF),
            pltpu.VMEM((4, 2 * NQ, 8, NG), BF),
            pltpu.VMEM((4, 2 * NQ, 8, NG), F32),
            pltpu.VMEM((STAGED, PC, 2, NQ // NX, 8, NG), BF),
            pltpu.VMEM((STAGED, PC, 2, NQ // NX, 8, NG), BF),
            pltpu.VMEM((STAGED, PC, 2, NQ // NX, 8, NG), F32),
            pltpu.VMEM((SLOTS // 4, 2, 8 * 2 * PC, 128), F32),
            pltpu.VMEM((SLOTS // 4, 4, RB, NG), BF),
            pltpu.VMEM((SLOTS, RB, NG), BF),
            pltpu.VMEM((NQ, 2, 128), F32),
            pltpu.VMEM((1, NG), jnp.int32),
            dma((len(STEPS),)),
            dma,
            dma,
            dma,
            dma((NC,)),
            dma((NC,)),
            dma,
            dma((4,)),
            dma,
            dma((NC,)),
            dma,
            dma,
            dma,
            dma,
            pltpu.SemaphoreType.REGULAR,
            pltpu.SemaphoreType.REGULAR,
            pltpu.SemaphoreType.REGULAR,
        ],
        compiler_params=pltpu.CompilerParams(collective_id=0, has_side_effects=True),
    )(samples.transpose(2, 0, 1), operator_rows, block_start, gauge_group.reshape(1, NG))
    return pl.pallas_call(
        finish,
        out_shape=(jax.ShapeDtypeStruct((1, 2, NF, NG), F32), jax.ShapeDtypeStruct((1, 2, NF, GROUPS), F32)),
        in_specs=[in_vmem] * 2,
        out_specs=(in_vmem, in_vmem),
    )(pltpu.with_memory_space_constraint(acc, pltpu.VMEM), pltpu.with_memory_space_constraint(seg, pltpu.VMEM))


def solution(mesh):
    return jax.shard_map(
        local,
        mesh=mesh,
        in_specs=(P("qoi", "param", None), P(None, "param", None, "qoi"), P(), P("qoi")),
        out_specs=(P("param", None, None, "qoi"), P("param", None, None, None)),
        check_vma=False,
    )
```
